32 devices in a mesh: pipe: 2 (over core), dp: 4 (over z), tensor: 4 (over y, x).
Axes of the slice: x: 2, y: 2, z: 4, core: 2. Of those that a mesh axis runs over, the one named last changes fastest.
Arguments:
- tokens: bfloat16 [2, 2048, 1536], P(None, ('dp', 'tensor')), may hold values from -6 to 6
- cotangent: bfloat16 [2, 2048, 1536], P(None, ('dp', 'tensor')), may hold values from -6 to 6
- w_query: bfloat16 [2, 1536, 1536], P('pipe', None, 'tensor'), may hold values from -0.15625 to 0.15625
- key_projection_weight: bfloat16 [2, 1536, 768], P('pipe', None, 'tensor'), may hold values from -0.15625 to 0.15625
- value_projection_weight: bfloat16 [2, 1536, 768], P('pipe', None, 'tensor'), may hold values from -0.15625 to 0.15625
- w_out: bfloat16 [2, 1536, 1536], P('pipe', 'tensor'), may hold values from -2.5 to 2.5
- w_gate: bfloat16 [2, 1536, 4096], P('pipe', None, 'tensor'), may hold values from -0.15625 to 0.15625
- w_up: bfloat16 [2, 1536, 4096], P('pipe', None, 'tensor'), may hold values from -0.15625 to 0.15625
- w_down: bfloat16 [2, 4096, 1536], P('pipe', 'tensor'), may hold values from -0.09375 to 0.09375
- gain_attn: float32 [2, 1536], P('pipe'), may hold values from 0.1 to 1.9
- gain_ffn: float32 [2, 1536], P('pipe'), may hold values from 0.1 to 1.9
Outputs:
- layer_out: bfloat16 [2, 2, 2048, 1536], P('pipe', None, ('dp', 'tensor'))
- layer_grad: bfloat16 [2, 2, 2048, 1536], P('pipe', None, ('dp', 'tensor'))
- grad_query: float32 [2, 1536, 1536], P('pipe', None, 'tensor')
- grad_key: float32 [2, 1536, 768], P('pipe', None, 'tensor')
- grad_value: float32 [2, 1536, 768], P('pipe', None, 'tensor')
- grad_out: float32 [2, 1536, 1536], P('pipe', 'tensor')
- grad_gate: float32 [2, 1536, 4096], P('pipe', None, 'tensor')
- grad_up: float32 [2, 1536, 4096], P('pipe', None, 'tensor')
- grad_down: float32 [2, 4096, 1536], P('pipe', 'tensor')
- grad_gain_attn: float32 [2, 1536], P('pipe')
- grad_gain_ffn: float32 [2, 1536], P('pipe')
The draws below stay inside these ranges and needn't reach their ends.
All inputs are finite; a program needn't handle non-finite values.
Results may differ from the reference program's by a relative error of at most 0.03.
Values may be sent and summed in bfloat16 or wider, within the bound.
A program may use at most 256 MiB of HBM per device.

```python
import math
import jax
import jax.numpy as jnp
from jax import lax

MODEL_WIDTH = 1536
QUERY_HEADS = 16
KEY_VALUE_HEADS = 8
HEAD_SIZE = 96
FF = 4096
CH = 512
LEN = 1024
SEQS = 4
NCH = 2
N_PIPE = 2


def level_of(own_key, dims, cuts, least, high):
    loudness, own = 1.0, jax.random.fold_in(own_key, 6)
    for axis_at, blocks in cuts:
        steps = jnp.exp(jax.random.uniform(jax.random.fold_in(own, axis_at), (blocks,), jnp.float32, least / len(cuts), high / len(cuts)))
        loudness = loudness * jnp.repeat(steps, dims[axis_at] // blocks).reshape([-1 if axis == axis_at else 1 for axis in range(len(dims))])
    return loudness


def centred(rng, extent, spread, most, cuts=(), kind=jnp.bfloat16):
    factor_of = level_of(rng, extent, cuts, -0.22, 0.18) if cuts else 1.0
    values = jax.random.normal(rng, extent, jnp.float32) * spread * factor_of
    return jnp.minimum(jnp.maximum(values, -most), most).astype(kind)


def setup_inputs(seed: int = 0) -> dict:
    key_list = jax.random.split(jax.random.key(seed), 12)
    tokens = centred(key_list[0], (NCH, SEQS * CH, MODEL_WIDTH), 1.0, 6.0, ((1, 16),))
    cotangent = centred(key_list[1], (NCH, SEQS * CH, MODEL_WIDTH), 1.0, 6.0, ((1, 16),))
    w_query = centred(key_list[2], (N_PIPE, MODEL_WIDTH, QUERY_HEADS * HEAD_SIZE), MODEL_WIDTH ** -0.5, 0.15625, ((0, 2), (2, 4)))
    key_projection_weight = centred(key_list[3], (N_PIPE, MODEL_WIDTH, KEY_VALUE_HEADS * HEAD_SIZE), MODEL_WIDTH ** -0.5, 0.15625, ((0, 2), (2, 4)))
    value_projection_weight = centred(key_list[4], (N_PIPE, MODEL_WIDTH, KEY_VALUE_HEADS * HEAD_SIZE), MODEL_WIDTH ** -0.5, 0.15625, ((0, 2), (2, 4)))
    w_out = centred(key_list[5], (N_PIPE, QUERY_HEADS * HEAD_SIZE, MODEL_WIDTH), (max(QUERY_HEADS * HEAD_SIZE // min(LEN, 256), 1)) ** -0.5, 2.5, ((0, 2), (1, 4)))
    w_gate = centred(key_list[6], (N_PIPE, MODEL_WIDTH, FF), MODEL_WIDTH ** -0.5, 0.15625, ((0, 2), (2, 4)))
    w_up = centred(key_list[7], (N_PIPE, MODEL_WIDTH, FF), MODEL_WIDTH ** -0.5, 0.15625, ((0, 2), (2, 4)))
    w_down = centred(key_list[8], (N_PIPE, FF, MODEL_WIDTH), FF ** -0.5, 0.09375, ((0, 2), (1, 4)))
    gain_attn = jnp.clip(1.0 + 0.18 * jax.random.normal(key_list[9], (N_PIPE, MODEL_WIDTH), jnp.float32), 0.1, 1.9)
    gain_ffn = jnp.clip(1.0 + 0.18 * jax.random.normal(key_list[10], (N_PIPE, MODEL_WIDTH), jnp.float32), 0.1, 1.9)
    return dict(tokens=tokens, cotangent=cotangent, w_query=w_query, key_projection_weight=key_projection_weight, value_projection_weight=value_projection_weight, w_out=w_out, w_gate=w_gate, w_up=w_up, w_down=w_down, gain_attn=gain_attn, gain_ffn=gain_ffn)


EPS = 1e-05
THETA = 100000.0
MASKED = -1e+30
HIGHEST = lax.Precision.HIGHEST

@jax.custom_vjp
def reduced_precision(v):
    return lax.optimization_barrier(v.astype(jnp.bfloat16)).astype(jnp.float32)

@jax.custom_vjp
def reduced_backward(v):
    return v

def low_keep(v):
    return (reduced_precision(v), None)

def low_pass(kept, grad):
    return (grad,)

def back_keep(v):
    return (v, None)

def back_low(kept, grad):
    return (reduced_precision(grad),)
reduced_precision.defvjp(low_keep, low_pass)
reduced_backward.defvjp(back_keep, back_low)

def matrix_product(left, right):
    return jnp.dot(left, right, precision=HIGHEST, preferred_element_type=jnp.float32)

def rms_scale(vectors, gain):
    return vectors * lax.rsqrt(lax.optimization_barrier(jnp.mean(vectors * vectors, axis=-1, keepdims=True)) + EPS) * gain

def rotations(token_length):
    half_size = HEAD_SIZE // 2
    frequency = 1.0 / THETA ** (jnp.arange(half_size, dtype=jnp.float32) * 2.0 / HEAD_SIZE)
    places = jnp.arange(token_length, dtype=jnp.float32)
    angles = places[:, None] * frequency[None, :]
    return (jnp.cos(angles), jnp.sin(angles))

def rotary_embedding(vectors, cosine_angles, sine_angles):
    half_size = vectors.shape[-1] // 2
    lower_half = vectors[..., :half_size]
    upper_half = vectors[..., half_size:]
    cosine_row = cosine_angles[:, None, :]
    sine_row = sine_angles[:, None, :]
    return jnp.concatenate([lower_half * cosine_row - upper_half * sine_row, upper_half * cosine_row + lower_half * sine_row], axis=-1)

def layer_pass(layer_input, weights, section_number, cosine_angles, sine_angles):
    w_query, key_projection_weight, value_projection_weight, w_out, w_gate, w_up, w_down, gain_attn, gain_ffn = weights
    token_length = layer_input.shape[0]
    heads_per_group = QUERY_HEADS // KEY_VALUE_HEADS
    normalized_input = reduced_precision(rms_scale(layer_input, gain_attn[section_number]))
    query_lin = reduced_backward(matrix_product(normalized_input, w_query[section_number]))
    key_linear = reduced_backward(matrix_product(normalized_input, key_projection_weight[section_number]))
    value_head_rows = reduced_precision(reduced_backward(matrix_product(normalized_input, value_projection_weight[section_number]))).reshape(token_length, KEY_VALUE_HEADS, HEAD_SIZE)
    query_rotated = reduced_precision(rotary_embedding(query_lin.reshape(token_length, QUERY_HEADS, HEAD_SIZE), cosine_angles, sine_angles))
    key_rotated = reduced_precision(rotary_embedding(key_linear.reshape(token_length, KEY_VALUE_HEADS, HEAD_SIZE), cosine_angles, sine_angles))
    grouped_heads = query_rotated.reshape(token_length, KEY_VALUE_HEADS, heads_per_group, HEAD_SIZE)
    scores = jnp.einsum('qkgd,tkd->kgqt', grouped_heads, key_rotated, precision=HIGHEST) * (1.0 / math.sqrt(HEAD_SIZE))
    causal = jnp.arange(token_length)[None, :] <= jnp.arange(token_length)[:, None]
    scores = reduced_backward(jnp.where(causal, scores, MASKED))
    row_max = lax.optimization_barrier(jnp.max(scores, axis=-1, keepdims=True))
    exponent = jnp.exp(scores - row_max)
    attention = reduced_precision(exponent / lax.optimization_barrier(jnp.sum(exponent, axis=-1, keepdims=True)))
    mixed_heads = jnp.einsum('kgqt,tkd->qkgd', attention, value_head_rows, precision=HIGHEST).reshape(token_length, QUERY_HEADS * HEAD_SIZE)
    mixed_heads = reduced_precision(reduced_backward(mixed_heads))
    residual = layer_input + reduced_backward(matrix_product(mixed_heads, w_out[section_number]))
    normed_two = reduced_precision(rms_scale(residual, gain_ffn[section_number]))
    gate_lin = reduced_backward(matrix_product(normed_two, w_gate[section_number]))
    up_lin = reduced_backward(matrix_product(normed_two, w_up[section_number]))
    hidden = reduced_precision(jax.nn.silu(gate_lin) * up_lin)
    return residual + reduced_backward(matrix_product(hidden, w_down[section_number]))

def forward(x_seq, zero_seq, weights):
    cosine_angles, sine_angles = rotations(LEN)

    def sequence_pass(scan_carry, pieces):
        layer_input, zero_input = pieces
        first_out = layer_pass(layer_input, weights, 0, cosine_angles, sine_angles)
        passed = reduced_backward(reduced_precision(first_out) + zero_input)
        return (scan_carry, (passed, layer_pass(passed, weights, 1, cosine_angles, sine_angles)))
    scan_carry, results = lax.scan(jax.checkpoint(sequence_pass), jnp.zeros((), jnp.float32), (x_seq, zero_seq))
    return results

def to_sequences(array):
    return array.reshape(LEN // CH, SEQS, CH, MODEL_WIDTH).transpose(1, 0, 2, 3).reshape(SEQS, LEN, MODEL_WIDTH)

def to_blocks(array):
    return array.reshape(SEQS, LEN // CH, CH, MODEL_WIDTH).transpose(1, 0, 2, 3).reshape(LEN // CH, SEQS * CH, MODEL_WIDTH)

def reference(tokens, cotangent, w_query, key_projection_weight, value_projection_weight, w_out, w_gate, w_up, w_down, gain_attn, gain_ffn):
    weights = (w_query.astype(jnp.float32), key_projection_weight.astype(jnp.float32), value_projection_weight.astype(jnp.float32), w_out.astype(jnp.float32), w_gate.astype(jnp.float32), w_up.astype(jnp.float32), w_down.astype(jnp.float32), gain_attn.astype(jnp.float32), gain_ffn.astype(jnp.float32))
    x_seq = to_sequences(tokens.astype(jnp.float32))
    zero_seq = jnp.zeros_like(x_seq)
    results, pullback = jax.vjp(forward, x_seq, zero_seq, weights)
    first_out, second_out = results
    grad_x, grad_zero, grad_w = pullback((jnp.zeros_like(first_out), to_sequences(cotangent.astype(jnp.float32))))
    layer_out = jnp.stack([to_blocks(first_out), to_blocks(second_out)]).astype(jnp.bfloat16)
    layer_grad = jnp.stack([to_blocks(grad_x), to_blocks(grad_zero)]).astype(jnp.bfloat16)
    return (layer_out, layer_grad, grad_w[0], grad_w[1], grad_w[2], grad_w[3], grad_w[4], grad_w[5], grad_w[6], grad_w[7], grad_w[8])
```

```python
import math

import jax
import jax.numpy as jnp
from jax import lax
from jax.sharding import PartitionSpec as P

MODEL_WIDTH = 1536
QUERY_HEADS = 16
KEY_VALUE_HEADS = 8
HEAD_SIZE = 96
CH = 512

EPS = 1e-05
THETA = 100000.0
MASKED = -1e30

TENSOR_X = [(t, t ^ 1) for t in range(4)]
TENSOR_Y = [(t, t ^ 2) for t in range(4)]
SWAP = [(0, 1), (1, 0)]


def product(left, right):
    return jnp.dot(left, right, preferred_element_type=jnp.float32)


def product_tn(left, right):
    return lax.dot_general(
        left, right, (((0,), (0,)), ((), ())), preferred_element_type=jnp.float32
    )


def product_nt(left, right):
    return lax.dot_general(
        left, right, (((1,), (1,)), ((), ())), preferred_element_type=jnp.float32
    )


def rms_scale(vectors, gain):
    return vectors * lax.rsqrt(jnp.mean(vectors * vectors, axis=-1, keepdims=True) + EPS) * gain


def rms_back(vectors, gain, gradient):
    inverse = lax.rsqrt(jnp.mean(vectors * vectors, axis=-1, keepdims=True) + EPS)
    unit_rows = vectors * inverse
    scaled = gradient * gain
    d_input = inverse * (scaled - unit_rows * jnp.mean(scaled * unit_rows, axis=-1, keepdims=True))
    return (d_input, jnp.sum(gradient * unit_rows, axis=0))


def gather_rows(own):
    half = own.shape[1] // 2
    one = lax.ppermute(own, "tensor", TENSOR_X)
    two = lax.ppermute(own, "tensor", TENSOR_Y)
    low = lax.ppermute(one[:, :half], "tensor", TENSOR_Y)
    high = lax.ppermute(two[:, half:], "tensor", TENSOR_X)
    return jnp.concatenate([own, one, two, jnp.concatenate([low, high], axis=1)], axis=0)


def scatter_rows(terms):
    rows = terms.shape[0] // 4
    half = terms.shape[1] // 2
    b = [terms[r * rows : (r + 1) * rows] for r in range(4)]
    send_x = jnp.concatenate([b[1][:, :half], b[3][:, :half]], axis=0)
    send_y = jnp.concatenate([b[2][:, half:], b[3][:, half:]], axis=0)
    got_x = lax.ppermute(send_x, "tensor", TENSOR_X).astype(jnp.float32)
    got_y = lax.ppermute(send_y, "tensor", TENSOR_Y).astype(jnp.float32)
    next_y = (b[2][:, :half].astype(jnp.float32) + got_x[rows:]).astype(jnp.bfloat16)
    next_x = (b[1][:, half:].astype(jnp.float32) + got_y[rows:]).astype(jnp.bfloat16)
    last_y = lax.ppermute(next_y, "tensor", TENSOR_Y).astype(jnp.float32)
    last_x = lax.ppermute(next_x, "tensor", TENSOR_X).astype(jnp.float32)
    low = b[0][:, :half].astype(jnp.float32) + got_x[:rows] + last_y
    high = b[0][:, half:].astype(jnp.float32) + got_y[:rows] + last_x
    return jnp.concatenate([low, high], axis=1)


def rotate(vectors, cosine, sine):
    half = vectors.shape[-1] // 2
    lower, upper = vectors[..., :half], vectors[..., half:]
    cosine, sine = cosine[:, None, :], sine[:, None, :]
    return jnp.concatenate([lower * cosine - upper * sine, upper * cosine + lower * sine], axis=-1)


def chain_steps(dp_size, owner):
    half = dp_size // 2
    at = lambda pairs: [(owner * dp_size + a, owner * dp_size + b) for a, b in pairs]
    inward = [at([(i, i + 1), (dp_size - 1 - i, dp_size - 2 - i)]) for i in range(half - 1)]
    across = at([(half - 1, half), (half, half - 1)])
    outward = [[(b, a) for a, b in pairs] for pairs in reversed(inward)]
    return inward, across, outward


def line_sum(term, owner):
    dp_size = lax.axis_size("dp")
    place = lax.axis_index("dp")
    half = dp_size // 2
    inward, across, outward = chain_steps(dp_size, owner)
    both = ("pipe", "dp")
    add = lambda a, b: (a.astype(jnp.float32) + b.astype(jnp.float32)).astype(jnp.bfloat16)
    total = add(term, lax.ppermute(term, "pipe", [(1 - owner, owner)]))
    for pairs in inward:
        total = add(total, lax.ppermute(total, both, pairs))
    total = add(total, lax.ppermute(total, both, across))
    for step, pairs in enumerate(outward):
        got = lax.ppermute(total, both, pairs)
        low, high = half - 2 - step, half + 1 + step
        total = jnp.where((place == low) | (place == high), got, total)
    return total


def body(
    tokens,
    cotangent,
    w_query,
    key_projection_weight,
    value_projection_weight,
    w_out,
    w_gate,
    w_up,
    w_down,
    gain_attn,
    gain_ffn,
):
    section = lax.axis_index("pipe")
    me = lax.axis_index("tensor")
    tensor = lax.axis_size("tensor")
    share = tokens.shape[1]
    rows = share * tensor
    assert tensor == 4 and rows == CH and tokens.shape[0] == 2
    heads = QUERY_HEADS // tensor
    groups = KEY_VALUE_HEADS // tensor
    per_group = heads // groups
    q_width, k_width = heads * HEAD_SIZE, groups * HEAD_SIZE
    f_width = w_gate.shape[2]
    scale = 1.0 / math.sqrt(HEAD_SIZE)
    first = section == 0

    def of_layers(own):
        other = lax.ppermute(own, "pipe", SWAP)
        return jnp.where(first, own, other), jnp.where(first, other, own)

    w_qkv = of_layers(
        jnp.concatenate([w_query[0], key_projection_weight[0], value_projection_weight[0]], axis=1)
    )
    w_o = of_layers(w_out[0])
    w_gu = of_layers(jnp.concatenate([w_gate[0], w_up[0]], axis=1))
    w_dn = of_layers(w_down[0])
    gains = of_layers(jnp.concatenate([gain_attn, gain_ffn], axis=0))

    inner = (me ^ jnp.arange(4, dtype=jnp.int32))[:, None] * share
    inner = (inner + jnp.arange(share, dtype=jnp.int32)[None, :]).reshape(rows)
    q_place = section * CH + inner
    k_place = jnp.concatenate([q_place, (1 - section) * CH + inner])
    mask = k_place[None, :] <= q_place[:, None]
    frequency = 1.0 / THETA ** (
        jnp.arange(HEAD_SIZE // 2, dtype=jnp.float32) * 2.0 / HEAD_SIZE
    )
    angles = q_place.astype(jnp.float32)[:, None] * frequency[None, :]
    cosine, sine = jnp.cos(angles), jnp.sin(angles)

    current = jnp.where(first, tokens[0], tokens[1])
    incoming = jnp.where(first, cotangent[0], cotangent[1])
    kept = []
    outputs = []
    for layer in range(2):
        u = current.astype(jnp.float32)
        n1 = gather_rows(rms_scale(u, gains[layer][0]).astype(jnp.bfloat16))
        projected = product(n1, w_qkv[layer])
        q = rotate(projected[:, :q_width].reshape(rows, heads, HEAD_SIZE), cosine, sine)
        q = q.astype(jnp.bfloat16).reshape(rows, groups, per_group, HEAD_SIZE)
        k = rotate(
            projected[:, q_width : q_width + k_width].reshape(rows, groups, HEAD_SIZE), cosine, sine
        ).astype(jnp.bfloat16)
        v = projected[:, q_width + k_width :].astype(jnp.bfloat16)
        kv = jnp.concatenate([k.reshape(rows, k_width), v], axis=1)
        kv = jnp.concatenate([kv, lax.ppermute(kv, "pipe", SWAP)], axis=0)
        k = kv[:, :k_width].reshape(2 * rows, groups, HEAD_SIZE)
        v = kv[:, k_width:].reshape(2 * rows, groups, HEAD_SIZE)
        s = jnp.einsum("qkgd,tkd->kgqt", q, k, preferred_element_type=jnp.float32) * scale
        s = jnp.where(mask, s, MASKED)
        top = jnp.max(s, axis=-1, keepdims=True)
        e = jnp.exp(s - top)
        norm = jnp.sum(e, axis=-1, keepdims=True)
        probs = (e / norm).astype(jnp.bfloat16)
        log_norm = top + jnp.log(norm)
        o = jnp.einsum("kgqt,tkd->qkgd", probs, v, preferred_element_type=jnp.float32)
        o = o.astype(jnp.bfloat16).reshape(rows, q_width)
        r = u + scatter_rows(product(o, w_o[layer]).astype(jnp.bfloat16))
        n2 = gather_rows(rms_scale(r, gains[layer][1]).astype(jnp.bfloat16))
        gate_up = product(n2, w_gu[layer])
        gate, up = gate_up[:, :f_width], gate_up[:, f_width:]
        hid = (jax.nn.silu(gate) * up).astype(jnp.bfloat16)
        y = r + scatter_rows(product(hid, w_dn[layer]).astype(jnp.bfloat16))
        current = y.astype(jnp.bfloat16)
        outputs.append(current)
        kept.append((u, n1, q, k, v, log_norm, o, r, n2, gate, up, hid))

    sums = [None, None]
    gain_terms = [None, None]
    grads_out = [None, None]
    for layer in (1, 0):
        u, n1, q, k, v, log_norm, o, r, n2, gate, up, hid = kept[layer]
        g = incoming.astype(jnp.float32)
        g_all = gather_rows(incoming)
        t_down = product_tn(hid, g_all).astype(jnp.bfloat16)
        d_hid = product_nt(g_all, w_dn[layer])
        sig = jax.nn.sigmoid(gate)
        d_gate = d_hid * up * sig * (1.0 + gate * (1.0 - sig))
        d_up = d_hid * gate * sig
        d_gu = jnp.concatenate([d_gate, d_up], axis=1).astype(jnp.bfloat16)
        t_gu = product_tn(n2, d_gu).astype(jnp.bfloat16)
        d_n2 = scatter_rows(product_nt(d_gu, w_gu[layer]).astype(jnp.bfloat16))
        back, d_gain_two = rms_back(r, gains[layer][1], d_n2)
        d_r = g + back
        d_attn = gather_rows(d_r.astype(jnp.bfloat16))
        t_out = product_tn(o, d_attn).astype(jnp.bfloat16)
        d_o = product_nt(d_attn, w_o[layer]).astype(jnp.bfloat16)
        d_o = d_o.reshape(rows, groups, per_group, HEAD_SIZE)
        s = jnp.einsum("qkgd,tkd->kgqt", q, k, preferred_element_type=jnp.float32) * scale
        probs = jnp.exp(jnp.where(mask, s, MASKED) - log_norm)
        d_p = jnp.einsum("qkgd,tkd->kgqt", d_o, v, preferred_element_type=jnp.float32)
        inner_sum = jnp.sum(probs * d_p, axis=-1, keepdims=True)
        d_s = (probs * (d_p - inner_sum)).astype(jnp.bfloat16)
        d_q = jnp.einsum("kgqt,tkd->qkgd", d_s, k, preferred_element_type=jnp.float32) * scale
        d_k = jnp.einsum("kgqt,qkgd->tkd", d_s, q, preferred_element_type=jnp.float32) * scale
        d_v = jnp.einsum(
            "kgqt,qkgd->tkd", probs.astype(jnp.bfloat16), d_o, preferred_element_type=jnp.float32
        )
        d_kv = jnp.concatenate(
            [d_k.reshape(2 * rows, k_width), d_v.reshape(2 * rows, k_width)], axis=1
        )
        d_kv = d_kv[:rows] + lax.ppermute(d_kv[rows:], "pipe", SWAP)
        d_q = rotate(d_q.reshape(rows, heads, HEAD_SIZE), cosine, -sine)
        d_k = rotate(d_kv[:, :k_width].reshape(rows, groups, HEAD_SIZE), cosine, -sine)
        d_qkv = jnp.concatenate(
            [d_q.reshape(rows, q_width), d_k.reshape(rows, k_width), d_kv[:, k_width:]], axis=1
        ).astype(jnp.bfloat16)
        t_qkv = product_tn(n1, d_qkv).astype(jnp.bfloat16)
        d_n1 = scatter_rows(product_nt(d_qkv, w_qkv[layer]).astype(jnp.bfloat16))
        back, d_gain_one = rms_back(u, gains[layer][0], d_n1)
        incoming = (d_r + back).astype(jnp.bfloat16)
        grads_out[layer] = incoming
        gain_terms[layer] = jnp.stack([d_gain_one, d_gain_two])
        sums[layer] = [line_sum(term, layer) for term in (t_down, t_gu, t_out, t_qkv)]

    gain_sum = lax.psum(jnp.stack(gain_terms), ("pipe", "dp", "tensor"))
    gain_sum = jnp.where(first, gain_sum[0], gain_sum[1])
    down, gu, out, qkv = (
        jnp.where(first, a, b).astype(jnp.float32) for a, b in zip(sums[0], sums[1])
    )

    def by_section(pair):
        mine = jnp.where(first, pair[0], pair[1])
        theirs = lax.ppermute(jnp.where(first, pair[1], pair[0]), "pipe", SWAP)
        return jnp.stack([jnp.where(first, mine, theirs), jnp.where(first, theirs, mine)])[None]

    return (
        by_section(outputs),
        by_section(grads_out),
        qkv[:, :q_width][None],
        qkv[:, q_width : q_width + k_width][None],
        qkv[:, q_width + k_width :][None],
        out[None],
        gu[:, :f_width][None],
        gu[:, f_width:][None],
        down[None],
        gain_sum[0][None],
        gain_sum[1][None],
    )


def solution(mesh):
    rows_spec = P(None, ("dp", "tensor"), None)
    by_column = P("pipe", None, "tensor")
    by_row = P("pipe", "tensor", None)
    kept_spec = P("pipe", None, ("dp", "tensor"), None)
    gain = P("pipe", None)
    weights = (by_column, by_column, by_column, by_row, by_column, by_column, by_row, gain, gain)
    return jax.shard_map(
        body,
        mesh=mesh,
        in_specs=(rows_spec, rows_spec) + weights,
        out_specs=(kept_spec, kept_spec) + weights,
        check_vma=False,
    )
```
